8 devices in a mesh: ty: 2 (over z, y), tx: 4 (over x, core).
Axes of the slice: x: 2, y: 2, z: 1, core: 2. Of those that a mesh axis runs over, the one named last changes fastest.
Arguments:
- w_one: float32 [4, 2, 4, 384, 1536], P('tx', 'ty')
- w_two: float32 [4, 2, 4, 1536, 384], P('tx', 'ty')
- inputs: bfloat16 [4, 2, 8, 2048, 384], P('tx', 'ty')
- targets: bfloat16 [4, 2, 8, 2048, 384], P('tx', 'ty')
Outputs:
- output 1: float32 [4, 2, 4, 384, 1536], P('tx', 'ty')
- output 2: float32 [4, 2, 4, 1536, 384], P('tx', 'ty')
- output 3: float32 [4, 2, 8], P('tx', 'ty')
All inputs are finite; a program needn't handle non-finite values.
Results may differ from the reference program's by a relative error of at most 0.00490311.
Values are sent between devices in bfloat16 or wider.
A program may use at most 1 GiB of HBM per device.

```python
import jax
import jax.numpy as jnp
from jax import lax

MODEL_WIDTH = 384
FFN_WIDTH = 1536
LAYERS = 4
NUM_STEPS = 8
LOCAL_ROWS = 2048
GRID_X = 4
GRID_Y = 2
NORM_EPS = 1e-6
LEARN_RATE = MODEL_WIDTH / (FFN_WIDTH * LAYERS)
REPLICAS = GRID_X * GRID_Y


def setup_inputs(seed: int = 0) -> dict:
    key_list = jax.random.split(jax.random.key(seed), 8)
    base_one = jax.random.normal(key_list[0], (LAYERS, MODEL_WIDTH, FFN_WIDTH), jnp.float32)
    own_one = jax.random.normal(key_list[1], (GRID_X, GRID_Y, LAYERS, MODEL_WIDTH, FFN_WIDTH), jnp.float32)
    base_two = jax.random.normal(key_list[2], (LAYERS, FFN_WIDTH, MODEL_WIDTH), jnp.float32)
    own_two = jax.random.normal(key_list[3], (GRID_X, GRID_Y, LAYERS, FFN_WIDTH, MODEL_WIDTH), jnp.float32)
    w_one = (base_one + 0.6 * own_one) * MODEL_WIDTH ** -0.5
    w_two = (base_two + 0.6 * own_two) * FFN_WIDTH ** -0.5
    data_shape = (GRID_X, GRID_Y, NUM_STEPS, LOCAL_ROWS, MODEL_WIDTH)
    scale_shape = (GRID_X, GRID_Y, NUM_STEPS, 1, 1)
    input_scale = jnp.exp2(jax.random.uniform(key_list[4], scale_shape, jnp.float32, -1.0, 1.0))
    target_scale = jnp.exp2(jax.random.uniform(key_list[5], scale_shape, jnp.float32, -1.0, 1.0))
    inputs = (jax.random.normal(key_list[6], data_shape, jnp.float32) * input_scale).astype(jnp.bfloat16)
    targets = (jax.random.normal(key_list[7], data_shape, jnp.float32) * target_scale).astype(jnp.bfloat16)
    return {"w_one": w_one, "w_two": w_two, "inputs": inputs, "targets": targets}


def rms_norm(hidden):
    hid_f = hidden.astype(jnp.float32)
    inv_rms = lax.rsqrt(jnp.mean(hid_f * hid_f, axis=-1, keepdims=True) + NORM_EPS)
    return (hid_f * inv_rms).astype(jnp.bfloat16)


def replica_loss(w_one, w_two, step_acts, step_goals):
    def layer_fn(hidden, weights):
        layer_one, layer_two = weights
        normed = rms_norm(hidden)
        pre_act = jnp.dot(normed, layer_one.astype(jnp.bfloat16), preferred_element_type=jnp.float32)
        hidden_act = jax.nn.gelu(pre_act).astype(jnp.bfloat16)
        mlp_out = jnp.dot(hidden_act, layer_two.astype(jnp.bfloat16), preferred_element_type=jnp.float32)
        return (hidden.astype(jnp.float32) + mlp_out).astype(jnp.bfloat16), None

    final_h, _ = lax.scan(layer_fn, step_acts, (w_one, w_two))
    error_term = final_h.astype(jnp.float32) - step_goals.astype(jnp.float32)
    return jnp.mean(error_term * error_term)


def gossip_mix(params):
    sent_copy = params.astype(jnp.bfloat16).astype(jnp.float32)
    mix_sum = params + jnp.roll(sent_copy, 1, axis=0)
    mix_sum = mix_sum + jnp.roll(sent_copy, -1, axis=0)
    mix_sum = mix_sum + jnp.roll(sent_copy, 1, axis=1)
    mix_sum = mix_sum + jnp.roll(sent_copy, -1, axis=1)
    return mix_sum / 5.0


def reference(w_one, w_two, inputs, targets):
    value_grad_fn = jax.value_and_grad(replica_loss, argnums=(0, 1))

    def replica_grads(operands):
        return value_grad_fn(operands[0], operands[1], operands[2], operands[3])

    def step_fn(params, step_batch):
        p_one, p_two = params
        step_acts, step_goals = step_batch
        flat_args = (
            p_one.reshape((REPLICAS,) + p_one.shape[2:]),
            p_two.reshape((REPLICAS,) + p_two.shape[2:]),
            step_acts.reshape((REPLICAS,) + step_acts.shape[2:]),
            step_goals.reshape((REPLICAS,) + step_goals.shape[2:]),
        )
        loss_vals, grad_pair = lax.map(replica_grads, flat_args)
        new_one = gossip_mix(p_one) - LEARN_RATE * grad_pair[0].reshape(p_one.shape)
        new_two = gossip_mix(p_two) - LEARN_RATE * grad_pair[1].reshape(p_two.shape)
        return (new_one, new_two), loss_vals.reshape(GRID_X, GRID_Y)

    step_data = (jnp.moveaxis(inputs, 2, 0), jnp.moveaxis(targets, 2, 0))
    final_pair, step_losses = lax.scan(step_fn, (w_one, w_two), step_data)
    return final_pair[0], final_pair[1], jnp.moveaxis(step_losses, 0, 2)
```

```python
import functools

import jax
import jax.numpy as jnp
from jax import lax
from jax.experimental import pallas as pl
from jax.experimental.pallas import tpu as pltpu
from jax.sharding import PartitionSpec as P

NORM_EPS = 1e-6
GELU_K = 0.7978845608028654
GELU_C = 0.044715
ROW_TILE = 512
COL_TILE = 512

F32 = jnp.float32
BF16 = jnp.bfloat16


def dot_nn(lhs, rhs):
    return lax.dot_general(lhs, rhs, (((1,), (0,)), ((), ())), preferred_element_type=F32)


def dot_nt(lhs, rhs):
    return lax.dot_general(lhs, rhs, (((1,), (1,)), ((), ())), preferred_element_type=F32)


def dot_tn(lhs, rhs):
    return lax.dot_general(lhs, rhs, (((0,), (0,)), ((), ())), preferred_element_type=F32)


def col_slices(width):
    tile = min(COL_TILE, width)
    return [slice(start, start + tile) for start in range(0, width, tile)]


def train_kernel(layers, total_rows, *refs):
    weight_refs = refs[:layers]
    act_ref, goal_ref, grad_ref, loss_ref = refs[layers : layers + 4]
    weights, grad_sum, stage, hid, norm, act, slope, diff, load_sem, store_sem = refs[layers + 4 :]
    tile_idx = pl.program_id(0)
    last_tile = pl.num_programs(0) - 1
    dim, ffn = weights.shape[2], weights.shape[3]
    columns = col_slices(ffn)

    loads = [pltpu.make_async_copy(weight_refs[idx], weights.at[idx], load_sem.at[idx]) for idx in range(layers)]

    @pl.when(tile_idx == 0)
    def _():
        for load in loads:
            load.start()
        loss_ref[...] = jnp.zeros_like(loss_ref)
        for load in loads:
            load.wait()

    hid[0] = act_ref[...]

    def forward(layer, _):
        hid_f = hid[layer].astype(F32)
        inv = lax.rsqrt(jnp.mean(hid_f * hid_f, axis=-1, keepdims=True) + NORM_EPS)
        normed = (hid_f * inv).astype(BF16)
        norm[layer] = normed
        for cols in columns:
            pre = dot_nn(normed, weights[layer, 0, :, cols])
            sq = pre * pre
            tan = jnp.tanh(pre * (GELU_K + (GELU_K * GELU_C) * sq))
            half = 0.5 * pre
            act[layer, :, cols] = (half + half * tan).astype(BF16)
            slope[layer, :, cols] = (0.5 + 0.5 * tan) + half * (1.0 - tan * tan) * (GELU_K + (3.0 * GELU_K * GELU_C) * sq)
        mlp = dot_nt(act[layer], weights[layer, 1])
        hid[layer + 1] = (hid_f + mlp).astype(BF16)
        return 0

    lax.fori_loop(0, layers, forward, 0)

    err = hid[layers].astype(F32) - goal_ref[...].astype(F32)
    loss_ref[...] += jnp.sum(err * err, axis=0, keepdims=True)
    diff[...] = (err * (2.0 / (total_rows * dim))).astype(BF16)

    def backward(rev, _):
        layer = layers - 1 - rev
        grad_out = diff[...]
        normed = norm[layer]
        first = tile_idx == 0
        back = None
        for cols in columns:
            d_act = dot_nn(grad_out, weights[layer, 1, :, cols]).astype(BF16).astype(F32)
            d_pre = (d_act * slope[layer, :, cols]).astype(BF16)
            part_two = dot_tn(grad_out, act[layer, :, cols])
            part_one = dot_tn(normed, d_pre)

            @pl.when(first)
            def _():
                grad_sum[layer, 0, :, cols] = part_one
                grad_sum[layer, 1, :, cols] = part_two

            @pl.when(jnp.logical_not(first))
            def _():
                grad_sum[layer, 0, :, cols] += part_one
                grad_sum[layer, 1, :, cols] += part_two

            part = dot_nt(d_pre, weights[layer, 0, :, cols])
            back = part if back is None else back + part
        d_norm = back.astype(BF16).astype(F32)
        hid_f = hid[layer].astype(F32)
        inv = lax.rsqrt(jnp.mean(hid_f * hid_f, axis=-1, keepdims=True) + NORM_EPS)
        mean_dot = jnp.mean(hid_f * d_norm, axis=-1, keepdims=True)
        d_in = inv * d_norm - hid_f * (mean_dot * (inv * inv * inv))
        diff[...] = (grad_out.astype(F32) + d_in).astype(BF16)

        @pl.when(tile_idx == last_tile)
        def _():
            slot = lax.rem(rev, 2)

            @pl.when(rev >= 2)
            def _():
                pltpu.make_async_copy(stage.at[slot], grad_ref.at[layer + 2], store_sem.at[slot]).wait()

            stage[slot] = grad_sum[layer].astype(BF16)
            pltpu.make_async_copy(stage.at[slot], grad_ref.at[layer], store_sem.at[slot]).start()

        return 0

    lax.fori_loop(0, layers, backward, 0)

    @pl.when(tile_idx == last_tile)
    def _():
        for rev in range(max(layers - 2, 0), layers):
            pltpu.make_async_copy(stage.at[rev % 2], grad_ref.at[layers - 1 - rev], store_sem.at[rev % 2]).wait()


def train_step(weight_list, inputs, targets, step_idx):
    layers = len(weight_list)
    _, dim, ffn = weight_list[0].shape
    rows = inputs.shape[3]
    tile = min(ROW_TILE, rows)
    any_spec = pl.BlockSpec(memory_space=pl.ANY)
    row_spec = pl.BlockSpec((None, None, None, tile, dim), lambda idx: (0, 0, step_idx, idx, 0))
    flops = 2 * rows * dim * ffn * (6 * layers)
    return pl.pallas_call(
        functools.partial(train_kernel, layers, rows),
        grid=(rows // tile,),
        out_shape=(
            jax.ShapeDtypeStruct((layers, 2, dim, ffn), BF16),
            jax.ShapeDtypeStruct((1, dim), F32),
        ),
        in_specs=[any_spec] * layers + [row_spec, row_spec],
        out_specs=(any_spec, pl.BlockSpec((1, dim), lambda idx: (0, 0))),
        scratch_shapes=[
            pltpu.VMEM((layers, 2, dim, ffn), BF16),
            pltpu.VMEM((layers, 2, dim, ffn), F32),
            pltpu.VMEM((2, 2, dim, ffn), BF16),
            pltpu.VMEM((layers + 1, tile, dim), BF16),
            pltpu.VMEM((layers, tile, dim), BF16),
            pltpu.VMEM((layers, tile, ffn), BF16),
            pltpu.VMEM((layers, tile, ffn), F32),
            pltpu.VMEM((tile, dim), BF16),
            pltpu.SemaphoreType.DMA((layers,)),
            pltpu.SemaphoreType.DMA((2,)),
        ],
        compiler_params=pltpu.CompilerParams(vmem_limit_bytes=63 * 2**20),
        cost_estimate=pl.CostEstimate(flops=flops, bytes_accessed=30 * 2**20, transcendentals=rows * ffn * layers),
        name="train_step",
    )(*weight_list, inputs, targets)


def cast_kernel(one_ref, two_ref, *rest):
    out_ref = rest[-1]
    out_ref[0] = one_ref[...].astype(BF16)
    out_ref[1] = two_ref[...].T.astype(BF16)


def stacked_specs(layer, dim, tile):
    one = pl.BlockSpec((None, None, None, dim, tile), lambda idx: (0, 0, layer, 0, idx))
    two = pl.BlockSpec((None, None, None, tile, dim), lambda idx: (0, 0, layer, idx, 0))
    return one, two


def first_cast(w_one, w_two, layer, after):
    dim, ffn = w_one.shape[3], w_one.shape[4]
    tile = min(COL_TILE, ffn)
    one, two = stacked_specs(layer, dim, tile)
    extra = [] if after is None else [after]
    return pl.pallas_call(
        cast_kernel,
        grid=(ffn // tile,),
        out_shape=jax.ShapeDtypeStruct((2, dim, ffn), BF16),
        in_specs=[one, two] + [pl.BlockSpec(memory_space=pl.ANY)] * len(extra),
        out_specs=pl.BlockSpec((2, dim, tile), lambda idx: (0, 0, idx)),
        cost_estimate=pl.CostEstimate(flops=6 * dim * ffn, bytes_accessed=12 * dim * ffn, transcendentals=0),
        name="first_cast",
    )(w_one, w_two, *extra)


def update_kernel(first, last, n_extra, lr, *refs):
    n_master = 2 if first else 1
    master = refs[:n_master]
    from_prev, from_next, from_y, grad = refs[n_master : n_master + 4]
    outs = refs[n_master + 4 + n_extra :]
    for part in range(2):
        if not first:
            value = master[0][part]
        elif part == 0:
            value = master[0][...]
        else:
            value = master[1][...].T
        far = from_y[part].astype(F32)
        value = value + from_prev[part].astype(F32)
        value = value + from_next[part].astype(F32)
        value = value + far
        value = value + far
        value = value / 5.0 - lr * grad[part].astype(F32)
        if not last:
            outs[0][part] = value
            outs[1][part] = value.astype(BF16)
        elif part == 0:
            outs[0][...] = value
        else:
            outs[1][...] = value.T


def update_layer(first, last, lr, layer, masters, received, grads, results, after):
    dim, ffn = grads.shape[2], grads.shape[3]
    layers = grads.shape[0]
    tile = min(COL_TILE, ffn)
    flat = pl.BlockSpec((2, dim, tile), lambda idx: (0, 0, idx))
    any_spec = pl.BlockSpec(memory_space=pl.ANY)
    one, two = stacked_specs(layer, dim, tile)
    master_specs = [one, two] if first else [flat]
    operands = list(masters) + list(received) + [grads]
    specs = master_specs + [flat] * 3 + [pl.BlockSpec((None, 2, dim, tile), lambda idx: (layer, 0, 0, idx))]
    extra = list(after)
    aliases = {}
    if last:
        if results is not None:
            aliases = {len(operands) + idx: idx for idx in range(2)}
            extra = list(results) + extra
        out_shape = (
            jax.ShapeDtypeStruct((1, 1, layers, dim, ffn), F32),
            jax.ShapeDtypeStruct((1, 1, layers, ffn, dim), F32),
        )
        out_specs = (one, two)
    else:
        out_shape = (jax.ShapeDtypeStruct((2, dim, ffn), F32), jax.ShapeDtypeStruct((2, dim, ffn), BF16))
        out_specs = (flat, flat)
    return pl.pallas_call(
        functools.partial(update_kernel, first, last, len(extra), lr),
        grid=(ffn // tile,),
        out_shape=out_shape,
        in_specs=specs + [any_spec] * len(extra),
        out_specs=out_specs,
        input_output_aliases=aliases,
        cost_estimate=pl.CostEstimate(flops=16 * dim * ffn, bytes_accessed=36 * dim * ffn, transcendentals=0),
        name="update_layer",
    )(*operands, *extra)


def neighbour_perms(grid_size):
    from_prev = [(src_idx, (src_idx + 1) % grid_size) for src_idx in range(grid_size)]
    from_next = [(src_idx, (src_idx - 1) % grid_size) for src_idx in range(grid_size)]
    return from_prev, from_next


def solution(mesh):
    prev_x, next_x = neighbour_perms(mesh.shape["tx"])
    prev_y, _ = neighbour_perms(mesh.shape["ty"])
    routes = [("tx", prev_x), ("tx", next_x), ("ty", prev_y)]

    def exchange(copy):
        return [lax.ppermute(copy, axis_name, pairs) for axis_name, pairs in routes]

    def device_train(w_one, w_two, inputs, targets):
        layers, dim, ffn = w_one.shape[2:]
        steps = inputs.shape[2]
        learn_rate = dim / (ffn * layers)
        order = list(range(layers))[::-1]
        copies = {}
        received = {}
        after = None
        for layer in order:
            copies[layer] = after = first_cast(w_one, w_two, layer, after)
            received[layer] = exchange(after)
        masters = {layer: (w_one, w_two) for layer in order}
        losses = []
        results = None
        for step_idx in range(steps):
            first, last = step_idx == 0, step_idx == steps - 1
            grads, loss = train_step([copies[layer] for layer in range(layers)], inputs, targets, step_idx)
            losses.append(loss)
            after = ()
            for layer in order:
                outs = update_layer(first, last, learn_rate, layer, masters[layer], received[layer], grads, results, after)
                if last:
                    results = outs
                else:
                    masters[layer] = (outs[0],)
                    copies[layer] = outs[1]
                    received[layer] = exchange(outs[1])
                    after = (outs[1],)
        loss_sum = jnp.sum(jnp.concatenate(losses, axis=0), axis=1) / (inputs.shape[3] * dim)
        return results[0], results[1], loss_sum[None, None]

    grid_spec = P("tx", "ty")
    return jax.shard_map(device_train, mesh=mesh, in_specs=(grid_spec,) * 4, out_specs=(grid_spec,) * 3, check_vma=False)
```

```python
import functools

import jax
import jax.numpy as jnp
from jax import lax
from jax.experimental import pallas as pl
from jax.experimental.pallas import tpu as pltpu
from jax.sharding import PartitionSpec as P

NORM_EPS = 1e-6
GELU_K = 0.7978845608028654
GELU_C = 0.044715
ROW_TILE = 512
COL_TILE = 512
HEAD_PIECES = (256, 512, 768)
TAIL_PIECES = (768, 512, 256)

F32 = jnp.float32
BF16 = jnp.bfloat16


def dot_nn(lhs, rhs):
    return lax.dot_general(lhs, rhs, (((1,), (0,)), ((), ())), preferred_element_type=F32)


def dot_nt(lhs, rhs):
    return lax.dot_general(lhs, rhs, (((1,), (1,)), ((), ())), preferred_element_type=F32)


def dot_tn(lhs, rhs):
    return lax.dot_general(lhs, rhs, (((0,), (0,)), ((), ())), preferred_element_type=F32)


def col_slices(width):
    tile = min(COL_TILE, width)
    return [slice(start, start + tile) for start in range(0, width, tile)]


def train_kernel(layers, places, total_rows, *refs):
    n_pieces = len(places)
    weight_refs = refs[:n_pieces]
    act_ref, goal_ref, grad_ref, loss_ref = refs[n_pieces : n_pieces + 4]
    weights, grad_sum, stage, hid, norm, act, slope, diff, load_sem, store_sem = refs[n_pieces + 4 :]
    tile_idx = pl.program_id(0)
    last_tile = pl.num_programs(0) - 1
    dim, ffn = weights.shape[2], weights.shape[3]
    columns = col_slices(ffn)

    loads = [
        pltpu.make_async_copy(weight_refs[idx], weights.at[layer, :, :, start : start + width], load_sem.at[idx])
        for idx, (layer, start, width) in enumerate(places)
    ]

    @pl.when(tile_idx == 0)
    def _():
        for load in loads:
            load.start()
        loss_ref[...] = jnp.zeros_like(loss_ref)
        for load in loads:
            load.wait()

    hid[0] = act_ref[...]

    def forward(layer, _):
        hid_f = hid[layer].astype(F32)
        inv = lax.rsqrt(jnp.mean(hid_f * hid_f, axis=-1, keepdims=True) + NORM_EPS)
        normed = (hid_f * inv).astype(BF16)
        norm[layer] = normed
        for cols in columns:
            pre = dot_nn(normed, weights[layer, 0, :, cols])
            sq = pre * pre
            tan = jnp.tanh(pre * (GELU_K + (GELU_K * GELU_C) * sq))
            half = 0.5 * pre
            act[layer, :, cols] = (half + half * tan).astype(BF16)
            slope[layer, :, cols] = (0.5 + 0.5 * tan) + half * (1.0 - tan * tan) * (GELU_K + (3.0 * GELU_K * GELU_C) * sq)
        mlp = dot_nt(act[layer], weights[layer, 1])
        hid[layer + 1] = (hid_f + mlp).astype(BF16)
        return 0

    lax.fori_loop(0, layers, forward, 0)

    err = hid[layers].astype(F32) - goal_ref[...].astype(F32)
    loss_ref[...] += jnp.sum(err * err, axis=0, keepdims=True)
    diff[...] = (err * (2.0 / (total_rows * dim))).astype(BF16)

    def backward(rev, _):
        layer = layers - 1 - rev
        grad_out = diff[...]
        normed = norm[layer]
        first = tile_idx == 0
        back = None
        for cols in columns:
            d_act = dot_nn(grad_out, weights[layer, 1, :, cols]).astype(BF16).astype(F32)
            d_pre = (d_act * slope[layer, :, cols]).astype(BF16)
            part_two = dot_tn(grad_out, act[layer, :, cols])
            part_one = dot_tn(normed, d_pre)

            @pl.when(first)
            def _():
                grad_sum[layer, 0, :, cols] = part_one
                grad_sum[layer, 1, :, cols] = part_two

            @pl.when(jnp.logical_not(first))
            def _():
                grad_sum[layer, 0, :, cols] += part_one
                grad_sum[layer, 1, :, cols] += part_two

            part = dot_nt(d_pre, weights[layer, 0, :, cols])
            back = part if back is None else back + part
        d_norm = back.astype(BF16).astype(F32)
        hid_f = hid[layer].astype(F32)
        inv = lax.rsqrt(jnp.mean(hid_f * hid_f, axis=-1, keepdims=True) + NORM_EPS)
        mean_dot = jnp.mean(hid_f * d_norm, axis=-1, keepdims=True)
        d_in = inv * d_norm - hid_f * (mean_dot * (inv * inv * inv))
        diff[...] = (grad_out.astype(F32) + d_in).astype(BF16)

        @pl.when(tile_idx == last_tile)
        def _():
            slot = lax.rem(rev, 2)

            @pl.when(rev >= 2)
            def _():
                pltpu.make_async_copy(stage.at[slot], grad_ref.at[layer + 2], store_sem.at[slot]).wait()

            stage[slot] = grad_sum[layer].astype(BF16)
            pltpu.make_async_copy(stage.at[slot], grad_ref.at[layer], store_sem.at[slot]).start()

        return 0

    lax.fori_loop(0, layers, backward, 0)

    @pl.when(tile_idx == last_tile)
    def _():
        for rev in range(max(layers - 2, 0), layers):
            pltpu.make_async_copy(stage.at[rev % 2], grad_ref.at[layers - 1 - rev], store_sem.at[rev % 2]).wait()


def train_step(copies, layers, ffn, inputs, targets, step_idx):
    places = [(layer, start, piece.shape[2]) for layer in range(layers) for start, piece in copies[layer]]
    weight_list = [piece for layer in range(layers) for _, piece in copies[layer]]
    dim = inputs.shape[4]
    rows = inputs.shape[3]
    tile = min(ROW_TILE, rows)
    any_spec = pl.BlockSpec(memory_space=pl.ANY)
    row_spec = pl.BlockSpec((None, None, None, tile, dim), lambda idx: (0, 0, step_idx, idx, 0))
    flops = 2 * rows * dim * ffn * (6 * layers)
    return pl.pallas_call(
        functools.partial(train_kernel, layers, places, rows),
        grid=(rows // tile,),
        out_shape=(
            jax.ShapeDtypeStruct((layers, 2, dim, ffn), BF16),
            jax.ShapeDtypeStruct((1, dim), F32),
        ),
        in_specs=[any_spec] * len(places) + [row_spec, row_spec],
        out_specs=(any_spec, pl.BlockSpec((1, dim), lambda idx: (0, 0))),
        scratch_shapes=[
            pltpu.VMEM((layers, 2, dim, ffn), BF16),
            pltpu.VMEM((layers, 2, dim, ffn), F32),
            pltpu.VMEM((2, 2, dim, ffn), BF16),
            pltpu.VMEM((layers + 1, tile, dim), BF16),
            pltpu.VMEM((layers, tile, dim), BF16),
            pltpu.VMEM((layers, tile, ffn), BF16),
            pltpu.VMEM((layers, tile, ffn), F32),
            pltpu.VMEM((tile, dim), BF16),
            pltpu.SemaphoreType.DMA((len(places),)),
            pltpu.SemaphoreType.DMA((2,)),
        ],
        compiler_params=pltpu.CompilerParams(vmem_limit_bytes=63 * 2**20),
        cost_estimate=pl.CostEstimate(flops=flops, bytes_accessed=30 * 2**20, transcendentals=rows * ffn * layers),
        name="train_step",
    )(*weight_list, inputs, targets)


def cast_kernel(one_ref, two_ref, *rest):
    out_ref = rest[-1]
    out_ref[0] = one_ref[...].astype(BF16)
    out_ref[1] = two_ref[...].T.astype(BF16)


def stacked_specs(layer, dim, tile, offset):
    one = pl.BlockSpec((None, None, None, dim, tile), lambda idx: (0, 0, layer, 0, offset + idx))
    two = pl.BlockSpec((None, None, None, tile, dim), lambda idx: (0, 0, layer, offset + idx, 0))
    return one, two


def tile_of(start, width):
    tile = next(size for size in (COL_TILE, COL_TILE // 2, 128) if start % size == 0 and width % size == 0)
    return tile, start // tile, width // tile


def first_cast(w_one, w_two, layer, piece, after):
    dim = w_one.shape[3]
    start, width = piece
    tile, offset, count = tile_of(start, width)
    one, two = stacked_specs(layer, dim, tile, offset)
    extra = [] if after is None else [after]
    return pl.pallas_call(
        cast_kernel,
        grid=(count,),
        out_shape=jax.ShapeDtypeStruct((2, dim, width), BF16),
        in_specs=[one, two] + [pl.BlockSpec(memory_space=pl.ANY)] * len(extra),
        out_specs=pl.BlockSpec((2, dim, tile), lambda idx: (0, 0, idx)),
        cost_estimate=pl.CostEstimate(flops=6 * dim * width, bytes_accessed=12 * dim * width, transcendentals=0),
        name="first_cast",
    )(w_one, w_two, *extra)


def update_kernel(first, last, n_extra, lr, *refs):
    n_master = 2 if first else 1
    master = refs[:n_master]
    from_prev, from_next, from_y, grad = refs[n_master : n_master + 4]
    outs = refs[n_master + 4 + n_extra :]
    for part in range(2):
        if not first:
            value = master[0][part]
        elif part == 0:
            value = master[0][...]
        else:
            value = master[1][...].T
        far = from_y[part].astype(F32)
        value = value + from_prev[part].astype(F32)
        value = value + from_next[part].astype(F32)
        value = value + far
        value = value + far
        value = value / 5.0 - lr * grad[part].astype(F32)
        if not last:
            outs[0][part] = value
            outs[1][part] = value.astype(BF16)
        elif part == 0:
            outs[0][...] = value
        else:
            outs[1][...] = value.T


def update_piece(first, last, lr, layer, piece, masters, received, grads, split, results, after):
    layers, _, dim, ffn = grads.shape
    start, width = piece
    tile, offset, count = tile_of(start, width)
    any_spec = pl.BlockSpec(memory_space=pl.ANY)

    def flat(base):
        return pl.BlockSpec((2, dim, tile), lambda idx: (0, 0, base + idx))

    one, two = stacked_specs(layer, dim, tile, offset)
    specs = [one, two] if first else [flat(offset - begin // tile) for begin, _ in masters]
    specs += [flat(offset - begin // tile) for begin, _ in received]
    specs.append(pl.BlockSpec((None, 2, dim, tile), lambda idx: (layer, 0, 0, offset + idx)))
    operands = [array for _, array in masters] + [array for _, array in received] + [grads]
    extra = list(after)
    aliases = {}
    if results is not None:
        aliases = {len(operands) + idx: idx for idx in range(2)}
        extra = list(results) + extra
    if last:
        out_shape = (
            jax.ShapeDtypeStruct((1, 1, layers, dim, ffn), F32),
            jax.ShapeDtypeStruct((1, 1, layers, ffn, dim), F32),
        )
        out_specs = (one, two)
    else:
        out_cols = width if split else ffn
        out_shape = (jax.ShapeDtypeStruct((2, dim, out_cols), F32), jax.ShapeDtypeStruct((2, dim, out_cols), BF16))
        out_specs = (flat(0 if split else offset),) * 2
    return pl.pallas_call(
        functools.partial(update_kernel, first, last, len(extra), lr),
        grid=(count,),
        out_shape=out_shape,
        in_specs=specs + [any_spec] * len(extra),
        out_specs=out_specs,
        input_output_aliases=aliases,
        cost_estimate=pl.CostEstimate(flops=16 * dim * width, bytes_accessed=36 * dim * width, transcendentals=0),
        name="update_layer",
    )(*operands, *extra)


def pieces_of(width, sizes):
    starts = [sum(sizes[:idx]) for idx in range(len(sizes))]
    return list(zip(starts, sizes)) if sum(sizes) == width else [(0, width)]


def neighbour_perms(grid_size):
    from_prev = [(src_idx, (src_idx + 1) % grid_size) for src_idx in range(grid_size)]
    from_next = [(src_idx, (src_idx - 1) % grid_size) for src_idx in range(grid_size)]
    return from_prev, from_next


def solution(mesh):
    prev_x, next_x = neighbour_perms(mesh.shape["tx"])
    prev_y, _ = neighbour_perms(mesh.shape["ty"])
    routes = [("tx", prev_x), ("tx", next_x), ("ty", prev_y)]

    def exchange(copy):
        return [lax.ppermute(copy, axis_name, pairs) for axis_name, pairs in routes]

    def device_train(w_one, w_two, inputs, targets):
        layers, dim, ffn = w_one.shape[2:]
        steps = inputs.shape[2]
        learn_rate = dim / (ffn * layers)
        order = list(range(layers))[::-1]
        whole = [(0, ffn)]
        head_pieces = pieces_of(ffn, HEAD_PIECES)
        tail_pieces = pieces_of(ffn, TAIL_PIECES)

        def exchanged(step_idx, layer):
            if step_idx == 0 and layer == order[0]:
                return head_pieces
            if step_idx == steps - 1 and layer == order[-1]:
                return tail_pieces
            return whole

        copies, received, masters = {}, {}, {}
        after = None
        for layer in order:
            copies[layer], received[layer] = [], []
            for piece in exchanged(0, layer):
                after = first_cast(w_one, w_two, layer, piece, after)
                copies[layer].append((piece[0], after))
                received[layer].append([(piece[0], array) for array in exchange(after)])
            masters[layer] = [[(0, w_one), (0, w_two)]]
        losses = []
        results = None
        after = ()
        for step_idx in range(steps):
            first, last = step_idx == 0, step_idx == steps - 1
            grads, loss = train_step(copies, layers, ffn, inputs, targets, step_idx)
            losses.append(loss)
            for layer in order:
                arrived = exchanged(step_idx, layer)
                leaving = whole if last else exchanged(step_idx + 1, layer)
                split = len(leaving) > 1
                old_masters, old_received = masters[layer], received[layer]
                if not last:
                    copies[layer], received[layer], masters[layer], results = [], [], [], None
                for idx, piece in enumerate(leaving if split else arrived):
                    own = old_masters[min(idx, len(old_masters) - 1)]
                    recv = old_received[min(idx, len(old_received) - 1)]
                    if results is not None:
                        after = ()
                    outs = update_piece(first, last, learn_rate, layer, piece, own, recv, grads, split, results, after)
                    if last or not split:
                        results = outs
                    if split:
                        copies[layer].append((piece[0], outs[1]))
                        masters[layer].append([(piece[0], outs[0])])
                        received[layer].append([(piece[0], array) for array in exchange(outs[1])])
                    after = () if last else (outs[1],)
                if not (last or split):
                    copies[layer].append((0, outs[1]))
                    masters[layer].append([(0, outs[0])])
                    received[layer].append([(0, array) for array in exchange(outs[1])])
            if not last:
                results = None
                after = ()
        loss_sum = jnp.sum(jnp.concatenate(losses, axis=0), axis=1) / (inputs.shape[3] * dim)
        return results[0], results[1], loss_sum[None, None]

    grid_spec = P("tx", "ty")
    return jax.shard_map(device_train, mesh=mesh, in_specs=(grid_spec,) * 4, out_specs=(grid_spec,) * 3, check_vma=False)
```

```python
import functools

import jax
import jax.numpy as jnp
from jax import lax
from jax.experimental import pallas as pl
from jax.experimental.pallas import tpu as pltpu
from jax.sharding import PartitionSpec as P

NORM_EPS = 1e-6
GELU_K = 0.7978845608028654
GELU_C = 0.044715
ROW_TILE = 512
COL_TILE = 512
MLP_TILE = 512
UPDATE_BLOCK = 128
ROW_BLOCK = 128
GRAD_BLOCK = 64
HEAD_PIECES = (256, 512, 768)
TAIL_PIECES = (768, 512, 256)

F32 = jnp.float32
BF16 = jnp.bfloat16


def dot_nn(lhs, rhs):
    return lax.dot_general(lhs, rhs, (((1,), (0,)), ((), ())), preferred_element_type=F32)


def dot_nt(lhs, rhs):
    return lax.dot_general(lhs, rhs, (((1,), (1,)), ((), ())), preferred_element_type=F32)


def dot_tn(lhs, rhs):
    return lax.dot_general(lhs, rhs, (((0,), (0,)), ((), ())), preferred_element_type=F32)


def each_block(count, size, body):
    def step(idx, _):
        body(pl.ds(pl.multiple_of(idx * size, size), size))
        return 0

    lax.fori_loop(0, count // size, step, 0)


def train_kernel(layers, places, total_rows, *refs):
    n_pieces = len(places)
    weight_refs = refs[:n_pieces]
    act_ref, goal_ref, grad_ref, loss_ref = refs[n_pieces : n_pieces + 4]
    weights, grad_sum, stage, hid, norm, act, slope, diff, total, load_sem, store_sem = refs[n_pieces + 4 :]
    tile_idx = pl.program_id(0)
    last_tile = pl.num_programs(0) - 1
    dim, ffn = weights.shape[2], weights.shape[3]
    tile = act_ref.shape[0]
    col_tile = min(MLP_TILE, ffn)
    chunks = ffn // col_tile

    loads = [
        pltpu.make_async_copy(weight_refs[idx], weights.at[layer, :, :, start : start + width], load_sem.at[idx])
        for idx, (layer, start, width) in enumerate(places)
    ]

    @pl.when(tile_idx == 0)
    def _():
        for load in loads:
            load.start()
        loss_ref[...] = jnp.zeros_like(loss_ref)

        def clear(layer, _):
            @functools.partial(each_block, dim, GRAD_BLOCK)
            def _(rows):
                grad_sum[layer, :, rows] = jnp.zeros((2, GRAD_BLOCK, ffn), F32)

            return 0

        lax.fori_loop(0, layers, clear, 0)
        for load in loads:
            load.wait()

    hid[0] = act_ref[...]

    def forward(layer, _):
        @functools.partial(each_block, tile, ROW_BLOCK)
        def _(rows):
            hid_f = hid[layer, rows].astype(F32)
            inv = lax.rsqrt(jnp.mean(hid_f * hid_f, axis=-1, keepdims=True) + NORM_EPS)
            norm[layer, rows] = (hid_f * inv).astype(BF16)
            total[rows] = hid_f

        def forward_columns(chunk, _):
            cols = pl.ds(pl.multiple_of(chunk * col_tile, col_tile), col_tile)
            pre = dot_nn(norm[layer], weights[layer, 0, :, cols])
            sq = pre * pre
            tan = jnp.tanh(pre * (GELU_K + (GELU_K * GELU_C) * sq))
            half = 0.5 * pre
            active = (half + half * tan).astype(BF16)
            act[layer, :, cols] = active
            slope[layer, :, cols] = (0.5 + 0.5 * tan) + half * (1.0 - tan * tan) * (GELU_K + (3.0 * GELU_K * GELU_C) * sq)
            total[...] += dot_nt(active, weights[layer, 1, :, cols])
            return 0

        lax.fori_loop(0, chunks, forward_columns, 0)

        @functools.partial(each_block, tile, ROW_BLOCK)
        def _(rows):
            hid[layer + 1, rows] = total[rows].astype(BF16)

        return 0

    lax.fori_loop(0, layers, forward, 0)

    @functools.partial(each_block, tile, ROW_BLOCK)
    def _(rows):
        err = hid[layers, rows].astype(F32) - goal_ref[rows].astype(F32)
        loss_ref[...] += jnp.sum(err * err, axis=0, keepdims=True)
        diff[rows] = (err * (2.0 / (total_rows * dim))).astype(BF16)

    def backward(rev, _):
        layer = layers - 1 - rev
        @functools.partial(each_block, tile, ROW_BLOCK)
        def _(rows):
            total[rows] = jnp.zeros((ROW_BLOCK, dim), F32)

        def backward_columns(chunk, _):
            cols = pl.ds(pl.multiple_of(chunk * col_tile, col_tile), col_tile)
            d_act = dot_nn(diff[...], weights[layer, 1, :, cols]).astype(BF16).astype(F32)
            d_pre = (d_act * slope[layer, :, cols]).astype(BF16)
            grad_sum[layer, 1, :, cols] += dot_tn(diff[...], act[layer, :, cols])
            grad_sum[layer, 0, :, cols] += dot_tn(norm[layer], d_pre)
            total[...] += dot_nt(d_pre, weights[layer, 0, :, cols])
            return 0

        lax.fori_loop(0, chunks, backward_columns, 0)

        @functools.partial(each_block, tile, ROW_BLOCK)
        def _(rows):
            d_norm = total[rows].astype(BF16).astype(F32)
            hid_f = hid[layer, rows].astype(F32)
            inv = lax.rsqrt(jnp.mean(hid_f * hid_f, axis=-1, keepdims=True) + NORM_EPS)
            mean_dot = jnp.mean(hid_f * d_norm, axis=-1, keepdims=True)
            d_in = inv * d_norm - hid_f * (mean_dot * (inv * inv * inv))
            diff[rows] = (diff[rows].astype(F32) + d_in).astype(BF16)

        @pl.when(tile_idx == last_tile)
        def _():
            slot = lax.rem(rev, 2)

            @pl.when(rev >= 2)
            def _():
                pltpu.make_async_copy(stage.at[slot], grad_ref.at[layer + 2], store_sem.at[slot]).wait()

            @functools.partial(each_block, dim, GRAD_BLOCK)
            def _(rows):
                stage[slot, :, rows] = grad_sum[layer, :, rows].astype(BF16)

            pltpu.make_async_copy(stage.at[slot], grad_ref.at[layer], store_sem.at[slot]).start()

        return 0

    lax.fori_loop(0, layers, backward, 0)

    @pl.when(tile_idx == last_tile)
    def _():
        for rev in range(max(layers - 2, 0), layers):
            pltpu.make_async_copy(stage.at[rev % 2], grad_ref.at[layers - 1 - rev], store_sem.at[rev % 2]).wait()


def train_step(copies, layers, ffn, inputs, targets, step_idx):
    places = [(layer, start, piece.shape[2]) for layer in range(layers) for start, piece in copies[layer]]
    weight_list = [piece for layer in range(layers) for _, piece in copies[layer]]
    dim = inputs.shape[4]
    rows = inputs.shape[3]
    tile = min(ROW_TILE, rows)
    any_spec = pl.BlockSpec(memory_space=pl.ANY)
    row_spec = pl.BlockSpec((None, None, None, tile, dim), lambda idx: (0, 0, step_idx, idx, 0))
    flops = 2 * rows * dim * ffn * (6 * layers)
    return pl.pallas_call(
        functools.partial(train_kernel, layers, places, rows),
        grid=(rows // tile,),
        out_shape=(
            jax.ShapeDtypeStruct((layers, 2, dim, ffn), BF16),
            jax.ShapeDtypeStruct((1, dim), F32),
        ),
        in_specs=[any_spec] * len(places) + [row_spec, row_spec],
        out_specs=(any_spec, pl.BlockSpec((1, dim), lambda idx: (0, 0))),
        scratch_shapes=[
            pltpu.VMEM((layers, 2, dim, ffn), BF16),
            pltpu.VMEM((layers, 2, dim, ffn), F32),
            pltpu.VMEM((2, 2, dim, ffn), BF16),
            pltpu.VMEM((layers + 1, tile, dim), BF16),
            pltpu.VMEM((layers, tile, dim), BF16),
            pltpu.VMEM((layers, tile, ffn), BF16),
            pltpu.VMEM((layers, tile, ffn), F32),
            pltpu.VMEM((tile, dim), BF16),
            pltpu.VMEM((tile, dim), F32),
            pltpu.SemaphoreType.DMA((len(places),)),
            pltpu.SemaphoreType.DMA((2,)),
        ],
        compiler_params=pltpu.CompilerParams(vmem_limit_bytes=63 * 2**20),
        cost_estimate=pl.CostEstimate(flops=flops, bytes_accessed=30 * 2**20, transcendentals=rows * ffn * layers),
        name="train_step",
    )(*weight_list, inputs, targets)


def cast_kernel(one_ref, two_ref, *rest):
    out_ref = rest[-1]
    out_ref[0] = one_ref[...].astype(BF16)
    out_ref[1] = two_ref[...].T.astype(BF16)


def stacked_specs(layer, dim, tile, offset):
    one = pl.BlockSpec((None, None, None, dim, tile), lambda idx: (0, 0, layer, 0, offset + idx))
    two = pl.BlockSpec((None, None, None, tile, dim), lambda idx: (0, 0, layer, offset + idx, 0))
    return one, two


def tile_of(start, width):
    tile = next(size for size in (COL_TILE, COL_TILE // 2, 128) if start % size == 0 and width % size == 0)
    return tile, start // tile, width // tile


def first_cast(w_one, w_two, layer, piece, after):
    dim = w_one.shape[3]
    start, width = piece
    tile, offset, count = tile_of(start, width)
    one, two = stacked_specs(layer, dim, tile, offset)
    extra = [] if after is None else [after]
    return pl.pallas_call(
        cast_kernel,
        grid=(count,),
        out_shape=jax.ShapeDtypeStruct((2, dim, width), BF16),
        in_specs=[one, two] + [pl.BlockSpec(memory_space=pl.ANY)] * len(extra),
        out_specs=pl.BlockSpec((2, dim, tile), lambda idx: (0, 0, idx)),
        cost_estimate=pl.CostEstimate(flops=6 * dim * width, bytes_accessed=12 * dim * width, transcendentals=0),
        name="first_cast",
    )(w_one, w_two, *extra)


def update_kernel(first, last, n_extra, lr, *refs):
    n_master = 2 if first else 1
    master = refs[:n_master]
    from_prev, from_next, from_y, grad = refs[n_master : n_master + 4]
    outs = refs[n_master + 4 + n_extra :]

    def mix(part, value, rows):
        far = from_y[part, rows].astype(F32)
        value = value + from_prev[part, rows].astype(F32)
        value = value + from_next[part, rows].astype(F32)
        value = value + far
        value = value + far
        return value / 5.0 - lr * grad[part, rows].astype(F32)

    @functools.partial(each_block, from_y.shape[1], UPDATE_BLOCK)
    def _(rows):
        for part in range(2):
            if not first:
                value = master[0][part, rows]
            elif part == 0:
                value = master[0][rows]
            else:
                value = master[1][:, rows].T
            value = mix(part, value, rows)
            if not last:
                outs[0][part, rows] = value
                outs[1][part, rows] = value.astype(BF16)
            elif part == 0:
                outs[0][rows] = value
            else:
                outs[1][:, rows] = value.T


def update_piece(first, last, lr, layer, piece, masters, received, grads, split, results, after):
    layers, _, dim, ffn = grads.shape
    start, width = piece
    tile, offset, count = tile_of(start, width)
    any_spec = pl.BlockSpec(memory_space=pl.ANY)

    def flat(base):
        return pl.BlockSpec((2, dim, tile), lambda idx: (0, 0, base + idx))

    one, two = stacked_specs(layer, dim, tile, offset)
    specs = [one, two] if first else [flat(offset - begin // tile) for begin, _ in masters]
    specs += [flat(offset - begin // tile) for begin, _ in received]
    specs.append(pl.BlockSpec((None, 2, dim, tile), lambda idx: (layer, 0, 0, offset + idx)))
    operands = [array for _, array in masters] + [array for _, array in received] + [grads]
    extra = list(after)
    aliases = {}
    if results is not None:
        aliases = {len(operands) + idx: idx for idx in range(2)}
        extra = list(results) + extra
    if last:
        out_shape = (
            jax.ShapeDtypeStruct((1, 1, layers, dim, ffn), F32),
            jax.ShapeDtypeStruct((1, 1, layers, ffn, dim), F32),
        )
        out_specs = (one, two)
    else:
        out_cols = width if split else ffn
        out_shape = (jax.ShapeDtypeStruct((2, dim, out_cols), F32), jax.ShapeDtypeStruct((2, dim, out_cols), BF16))
        out_specs = (flat(0 if split else offset),) * 2
    return pl.pallas_call(
        functools.partial(update_kernel, first, last, len(extra), lr),
        grid=(count,),
        out_shape=out_shape,
        in_specs=specs + [any_spec] * len(extra),
        out_specs=out_specs,
        input_output_aliases=aliases,
        cost_estimate=pl.CostEstimate(flops=16 * dim * width, bytes_accessed=36 * dim * width, transcendentals=0),
        name="update_layer",
    )(*operands, *extra)


def pieces_of(width, sizes):
    starts = [sum(sizes[:idx]) for idx in range(len(sizes))]
    return list(zip(starts, sizes)) if sum(sizes) == width else [(0, width)]


def neighbour_perms(grid_size):
    from_prev = [(src_idx, (src_idx + 1) % grid_size) for src_idx in range(grid_size)]
    from_next = [(src_idx, (src_idx - 1) % grid_size) for src_idx in range(grid_size)]
    return from_prev, from_next


def solution(mesh):
    prev_x, next_x = neighbour_perms(mesh.shape["tx"])
    prev_y, _ = neighbour_perms(mesh.shape["ty"])
    routes = [("tx", prev_x), ("tx", next_x), ("ty", prev_y)]

    def exchange(copy):
        return [lax.ppermute(copy, axis_name, pairs) for axis_name, pairs in routes]

    def device_train(w_one, w_two, inputs, targets):
        layers, dim, ffn = w_one.shape[2:]
        steps = inputs.shape[2]
        learn_rate = dim / (ffn * layers)
        order = list(range(layers))[::-1]
        whole = [(0, ffn)]
        head_pieces = pieces_of(ffn, HEAD_PIECES)
        tail_pieces = pieces_of(ffn, TAIL_PIECES)

        def exchanged(step_idx, layer):
            if step_idx == 0 and layer == order[0]:
                return head_pieces
            if step_idx == steps - 1 and layer == order[-1]:
                return tail_pieces
            return whole

        copies, received, masters = {}, {}, {}
        after = None
        for layer in order:
            copies[layer], received[layer] = [], []
            for piece in exchanged(0, layer):
                after = first_cast(w_one, w_two, layer, piece, after)
                copies[layer].append((piece[0], after))
                received[layer].append([(piece[0], array) for array in exchange(after)])
            masters[layer] = [[(0, w_one), (0, w_two)]]
        losses = []
        results = None
        after = ()
        for step_idx in range(steps):
            first, last = step_idx == 0, step_idx == steps - 1
            grads, loss = train_step(copies, layers, ffn, inputs, targets, step_idx)
            losses.append(loss)
            for layer in order:
                arrived = exchanged(step_idx, layer)
                leaving = whole if last else exchanged(step_idx + 1, layer)
                split = len(leaving) > 1
                old_masters, old_received = masters[layer], received[layer]
                if not last:
                    copies[layer], received[layer], masters[layer], results = [], [], [], None
                for idx, piece in enumerate(leaving if split else arrived):
                    own = old_masters[min(idx, len(old_masters) - 1)]
                    recv = old_received[min(idx, len(old_received) - 1)]
                    if results is not None:
                        after = ()
                    outs = update_piece(first, last, learn_rate, layer, piece, own, recv, grads, split, results, after)
                    if last or not split:
                        results = outs
                    if split:
                        copies[layer].append((piece[0], outs[1]))
                        masters[layer].append([(piece[0], outs[0])])
                        received[layer].append([(piece[0], array) for array in exchange(outs[1])])
                    after = () if last else (outs[1],)
                if not (last or split):
                    copies[layer].append((0, outs[1]))
                    masters[layer].append([(0, outs[0])])
                    received[layer].append([(0, array) for array in exchange(outs[1])])
            if not last:
                results = None
                after = ()
        loss_sum = jnp.sum(jnp.concatenate(losses, axis=0), axis=1) / (inputs.shape[3] * dim)
        return results[0], results[1], loss_sum[None, None]

    grid_spec = P("tx", "ty")
    return jax.shard_map(device_train, mesh=mesh, in_specs=(grid_spec,) * 4, out_specs=(grid_spec,) * 3, check_vma=False)
```

```python
import functools

import jax
import jax.numpy as jnp
from jax import lax
from jax.experimental import pallas as pl
from jax.experimental.pallas import tpu as pltpu
from jax.sharding import PartitionSpec as P

NORM_EPS = 1e-6
GELU_K = 0.7978845608028654
GELU_C = 0.044715
ROW_TILE = 512
COL_TILE = 512
MLP_TILE = 512
LAST_MLP_TILE = 768
UPDATE_BLOCK = 128
ROW_BLOCK = 128
GRAD_BLOCK = 32
HEAD_PIECES = (256, 512, 768)
TAIL_PIECES = (1024, 256, 128, 128)

F32 = jnp.float32
BF16 = jnp.bfloat16


def dot_nn(lhs, rhs):
    return lax.dot_general(lhs, rhs, (((1,), (0,)), ((), ())), preferred_element_type=F32)


def dot_nt(lhs, rhs):
    return lax.dot_general(lhs, rhs, (((1,), (1,)), ((), ())), preferred_element_type=F32)


def dot_tn(lhs, rhs):
    return lax.dot_general(lhs, rhs, (((0,), (0,)), ((), ())), preferred_element_type=F32)


def each_block(count, size, body):
    def step(idx, _):
        body(pl.ds(pl.multiple_of(idx * size, size), size))
        return 0

    lax.fori_loop(0, count // size, step, 0)


def train_kernel(layers, places, total_rows, mlp_tile, *refs):
    n_pieces = len(places)
    weight_refs = refs[:n_pieces]
    act_ref, goal_ref, grad_ref, loss_ref = refs[n_pieces : n_pieces + 4]
    weights, grad_sum, stage, hid, norm, act, slope, diff, total, load_sem, store_sem = refs[n_pieces + 4 :]
    tile_idx = pl.program_id(0)
    last_tile = pl.num_programs(0) - 1
    dim, ffn = weights.shape[2], weights.shape[3]
    tile = act_ref.shape[0]
    col_tile = min(mlp_tile, ffn)
    chunks = ffn // col_tile

    loads = [
        pltpu.make_async_copy(weight_refs[idx], weights.at[layer, :, :, start : start + width], load_sem.at[idx])
        for idx, (layer, start, width) in enumerate(places)
    ]

    @pl.when(tile_idx == 0)
    def _():
        for load in loads:
            load.start()
        loss_ref[...] = jnp.zeros_like(loss_ref)

        def clear(layer, _):
            @functools.partial(each_block, dim, GRAD_BLOCK)
            def _(rows):
                grad_sum[layer, :, rows] = jnp.zeros((2, GRAD_BLOCK, ffn), F32)

            return 0

        lax.fori_loop(0, layers, clear, 0)
        for load in loads:
            load.wait()

    hid[0] = act_ref[...]

    def forward(layer, _):
        @functools.partial(each_block, tile, ROW_BLOCK)
        def _(rows):
            hid_f = hid[layer, rows].astype(F32)
            inv = lax.rsqrt(jnp.mean(hid_f * hid_f, axis=-1, keepdims=True) + NORM_EPS)
            norm[layer, rows] = (hid_f * inv).astype(BF16)
            total[rows] = hid_f

        def forward_columns(chunk, _):
            cols = pl.ds(pl.multiple_of(chunk * col_tile, col_tile), col_tile)
            pre = dot_nn(norm[layer], weights[layer, 0, :, cols])
            sq = pre * pre
            tan = jnp.tanh(pre * (GELU_K + (GELU_K * GELU_C) * sq))
            half = 0.5 * pre
            active = (half + half * tan).astype(BF16)
            act[layer, :, cols] = active
            slope[layer, :, cols] = (0.5 + 0.5 * tan) + half * (1.0 - tan * tan) * (GELU_K + (3.0 * GELU_K * GELU_C) * sq)
            total[...] += dot_nt(active, weights[layer, 1, :, cols])
            return 0

        lax.fori_loop(0, chunks, forward_columns, 0)

        @functools.partial(each_block, tile, ROW_BLOCK)
        def _(rows):
            hid[layer + 1, rows] = total[rows].astype(BF16)

        return 0

    lax.fori_loop(0, layers, forward, 0)

    @functools.partial(each_block, tile, ROW_BLOCK)
    def _(rows):
        err = hid[layers, rows].astype(F32) - goal_ref[rows].astype(F32)
        loss_ref[...] += jnp.sum(err * err, axis=0, keepdims=True)
        diff[rows] = (err * (2.0 / (total_rows * dim))).astype(BF16)

    def backward(rev, _):
        layer = layers - 1 - rev
        @functools.partial(each_block, tile, ROW_BLOCK)
        def _(rows):
            total[rows] = jnp.zeros((ROW_BLOCK, dim), F32)

        def backward_columns(chunk, _):
            cols = pl.ds(pl.multiple_of(chunk * col_tile, col_tile), col_tile)
            d_act = dot_nn(diff[...], weights[layer, 1, :, cols]).astype(BF16).astype(F32)
            d_pre = (d_act * slope[layer, :, cols]).astype(BF16)
            grad_sum[layer, 1, :, cols] += dot_tn(diff[...], act[layer, :, cols])
            grad_sum[layer, 0, :, cols] += dot_tn(norm[layer], d_pre)
            total[...] += dot_nt(d_pre, weights[layer, 0, :, cols])
            return 0

        lax.fori_loop(0, chunks, backward_columns, 0)

        @functools.partial(each_block, tile, ROW_BLOCK)
        def _(rows):
            d_norm = total[rows].astype(BF16).astype(F32)
            hid_f = hid[layer, rows].astype(F32)
            inv = lax.rsqrt(jnp.mean(hid_f * hid_f, axis=-1, keepdims=True) + NORM_EPS)
            mean_dot = jnp.mean(hid_f * d_norm, axis=-1, keepdims=True)
            d_in = inv * d_norm - hid_f * (mean_dot * (inv * inv * inv))
            diff[rows] = (diff[rows].astype(F32) + d_in).astype(BF16)

        @pl.when(tile_idx == last_tile)
        def _():
            slot = lax.rem(rev, 2)

            @pl.when(rev >= 2)
            def _():
                pltpu.make_async_copy(stage.at[slot], grad_ref.at[layer + 2], store_sem.at[slot]).wait()

            @functools.partial(each_block, dim, GRAD_BLOCK)
            def _(rows):
                stage[slot, :, rows] = grad_sum[layer, :, rows].astype(BF16)

            pltpu.make_async_copy(stage.at[slot], grad_ref.at[layer], store_sem.at[slot]).start()

        return 0

    lax.fori_loop(0, layers, backward, 0)

    @pl.when(tile_idx == last_tile)
    def _():
        for rev in range(max(layers - 2, 0), layers):
            pltpu.make_async_copy(stage.at[rev % 2], grad_ref.at[layers - 1 - rev], store_sem.at[rev % 2]).wait()


def train_step(copies, layers, ffn, inputs, targets, step_idx):
    places = [(layer, start, piece.shape[2]) for layer in range(layers) for start, piece in copies[layer]]
    weight_list = [piece for layer in range(layers) for _, piece in copies[layer]]
    dim = inputs.shape[4]
    rows = inputs.shape[3]
    mlp_tile = LAST_MLP_TILE if step_idx == inputs.shape[2] - 1 else MLP_TILE
    tile = min(ROW_TILE, rows)
    any_spec = pl.BlockSpec(memory_space=pl.ANY)
    row_spec = pl.BlockSpec((None, None, None, tile, dim), lambda idx: (0, 0, step_idx, idx, 0))
    flops = 2 * rows * dim * ffn * (6 * layers)
    return pl.pallas_call(
        functools.partial(train_kernel, layers, places, rows, mlp_tile),
        grid=(rows // tile,),
        out_shape=(
            jax.ShapeDtypeStruct((layers, 2, dim, ffn), BF16),
            jax.ShapeDtypeStruct((1, dim), F32),
        ),
        in_specs=[any_spec] * len(places) + [row_spec, row_spec],
        out_specs=(any_spec, pl.BlockSpec((1, dim), lambda idx: (0, 0))),
        scratch_shapes=[
            pltpu.VMEM((layers, 2, dim, ffn), BF16),
            pltpu.VMEM((layers, 2, dim, ffn), F32),
            pltpu.VMEM((2, 2, dim, ffn), BF16),
            pltpu.VMEM((layers + 1, tile, dim), BF16),
            pltpu.VMEM((layers, tile, dim), BF16),
            pltpu.VMEM((layers, tile, ffn), BF16),
            pltpu.VMEM((layers, tile, ffn), F32),
            pltpu.VMEM((tile, dim), BF16),
            pltpu.VMEM((tile, dim), F32),
            pltpu.SemaphoreType.DMA((len(places),)),
            pltpu.SemaphoreType.DMA((2,)),
        ],
        compiler_params=pltpu.CompilerParams(vmem_limit_bytes=63 * 2**20),
        cost_estimate=pl.CostEstimate(flops=flops, bytes_accessed=30 * 2**20, transcendentals=rows * ffn * layers),
        name="train_step",
    )(*weight_list, inputs, targets)


def cast_kernel(one_ref, two_ref, *rest):
    out_ref = rest[-1]
    out_ref[0] = one_ref[...].astype(BF16)
    out_ref[1] = two_ref[...].T.astype(BF16)


def stacked_specs(layer, dim, tile, offset):
    one = pl.BlockSpec((None, None, None, dim, tile), lambda idx: (0, 0, layer, 0, offset + idx))
    two = pl.BlockSpec((None, None, None, tile, dim), lambda idx: (0, 0, layer, offset + idx, 0))
    return one, two


def tile_of(start, width):
    tile = next(size for size in (COL_TILE, COL_TILE // 2, 128) if start % size == 0 and width % size == 0)
    return tile, start // tile, width // tile


def first_cast(w_one, w_two, layer, piece, after):
    dim = w_one.shape[3]
    start, width = piece
    tile, offset, count = tile_of(start, width)
    one, two = stacked_specs(layer, dim, tile, offset)
    extra = [] if after is None else [after]
    return pl.pallas_call(
        cast_kernel,
        grid=(count,),
        out_shape=jax.ShapeDtypeStruct((2, dim, width), BF16),
        in_specs=[one, two] + [pl.BlockSpec(memory_space=pl.ANY)] * len(extra),
        out_specs=pl.BlockSpec((2, dim, tile), lambda idx: (0, 0, idx)),
        cost_estimate=pl.CostEstimate(flops=6 * dim * width, bytes_accessed=12 * dim * width, transcendentals=0),
        name="first_cast",
    )(w_one, w_two, *extra)


def update_kernel(first, last, n_extra, lr, *refs):
    n_master = 2 if first else 1
    master = refs[:n_master]
    from_prev, from_next, from_y, grad = refs[n_master : n_master + 4]
    outs = refs[n_master + 4 + n_extra :]

    def mix(part, value, rows):
        far = from_y[part, rows].astype(F32)
        value = value + from_prev[part, rows].astype(F32)
        value = value + from_next[part, rows].astype(F32)
        value = value + far
        value = value + far
        return value / 5.0 - lr * grad[part, rows].astype(F32)

    @functools.partial(each_block, from_y.shape[1], UPDATE_BLOCK)
    def _(rows):
        for part in range(2):
            if not first:
                value = master[0][part, rows]
            elif part == 0:
                value = master[0][rows]
            else:
                value = master[1][:, rows].T
            value = mix(part, value, rows)
            if not last:
                outs[0][part, rows] = value
                outs[1][part, rows] = value.astype(BF16)
            elif part == 0:
                outs[0][rows] = value
            else:
                outs[1][:, rows] = value.T


def update_piece(first, last, lr, layer, piece, masters, received, grads, split, results, after):
    layers, _, dim, ffn = grads.shape
    start, width = piece
    tile, offset, count = tile_of(start, width)
    any_spec = pl.BlockSpec(memory_space=pl.ANY)

    def flat(base):
        return pl.BlockSpec((2, dim, tile), lambda idx: (0, 0, base + idx))

    one, two = stacked_specs(layer, dim, tile, offset)
    specs = [one, two] if first else [flat(offset - begin // tile) for begin, _ in masters]
    specs += [flat(offset - begin // tile) for begin, _ in received]
    specs.append(pl.BlockSpec((None, 2, dim, tile), lambda idx: (layer, 0, 0, offset + idx)))
    operands = [array for _, array in masters] + [array for _, array in received] + [grads]
    extra = list(after)
    aliases = {}
    if results is not None:
        aliases = {len(operands) + idx: idx for idx in range(2)}
        extra = list(results) + extra
    if last:
        out_shape = (
            jax.ShapeDtypeStruct((1, 1, layers, dim, ffn), F32),
            jax.ShapeDtypeStruct((1, 1, layers, ffn, dim), F32),
        )
        out_specs = (one, two)
    else:
        out_cols = width if split else ffn
        out_shape = (jax.ShapeDtypeStruct((2, dim, out_cols), F32), jax.ShapeDtypeStruct((2, dim, out_cols), BF16))
        out_specs = (flat(0 if split else offset),) * 2
    return pl.pallas_call(
        functools.partial(update_kernel, first, last, len(extra), lr),
        grid=(count,),
        out_shape=out_shape,
        in_specs=specs + [any_spec] * len(extra),
        out_specs=out_specs,
        input_output_aliases=aliases,
        cost_estimate=pl.CostEstimate(flops=16 * dim * width, bytes_accessed=36 * dim * width, transcendentals=0),
        name="update_layer",
    )(*operands, *extra)


def pieces_of(width, sizes):
    starts = [sum(sizes[:idx]) for idx in range(len(sizes))]
    return list(zip(starts, sizes)) if sum(sizes) == width else [(0, width)]


def neighbour_perms(grid_size):
    from_prev = [(src_idx, (src_idx + 1) % grid_size) for src_idx in range(grid_size)]
    from_next = [(src_idx, (src_idx - 1) % grid_size) for src_idx in range(grid_size)]
    return from_prev, from_next


def solution(mesh):
    prev_x, next_x = neighbour_perms(mesh.shape["tx"])
    prev_y, _ = neighbour_perms(mesh.shape["ty"])
    routes = [("tx", prev_x), ("tx", next_x), ("ty", prev_y)]

    def exchange(copy):
        return [lax.ppermute(copy, axis_name, pairs) for axis_name, pairs in routes]

    def device_train(w_one, w_two, inputs, targets):
        layers, dim, ffn = w_one.shape[2:]
        steps = inputs.shape[2]
        learn_rate = dim / (ffn * layers)
        order = list(range(layers))[::-1]
        whole = [(0, ffn)]
        head_pieces = pieces_of(ffn, HEAD_PIECES)
        tail_pieces = pieces_of(ffn, TAIL_PIECES)

        def exchanged(step_idx, layer):
            if step_idx == 0 and layer == order[0]:
                return head_pieces
            if step_idx == steps - 1 and layer == order[-1]:
                return tail_pieces
            return whole

        copies, received, masters = {}, {}, {}
        after = None
        for layer in order:
            copies[layer], received[layer] = [], []
            for piece in exchanged(0, layer):
                after = first_cast(w_one, w_two, layer, piece, after)
                copies[layer].append((piece[0], after))
                received[layer].append([(piece[0], array) for array in exchange(after)])
            masters[layer] = [[(0, w_one), (0, w_two)]]
        losses = []
        results = None
        after = ()
        for step_idx in range(steps):
            first, last = step_idx == 0, step_idx == steps - 1
            grads, loss = train_step(copies, layers, ffn, inputs, targets, step_idx)
            losses.append(loss)
            for layer in order:
                arrived = exchanged(step_idx, layer)
                leaving = whole if last else exchanged(step_idx + 1, layer)
                split = len(leaving) > 1
                old_masters, old_received = masters[layer], received[layer]
                if not last:
                    copies[layer], received[layer], masters[layer], results = [], [], [], None
                for idx, piece in enumerate(leaving if split else arrived):
                    own = old_masters[min(idx, len(old_masters) - 1)]
                    recv = old_received[min(idx, len(old_received) - 1)]
                    if results is not None:
                        after = ()
                    outs = update_piece(first, last, learn_rate, layer, piece, own, recv, grads, split, results, after)
                    if last or not split:
                        results = outs
                    if split:
                        copies[layer].append((piece[0], outs[1]))
                        masters[layer].append([(piece[0], outs[0])])
                        received[layer].append([(piece[0], array) for array in exchange(outs[1])])
                    after = () if last else (outs[1],)
                if not (last or split):
                    copies[layer].append((0, outs[1]))
                    masters[layer].append([(0, outs[0])])
                    received[layer].append([(0, array) for array in exchange(outs[1])])
            if not last:
                results = None
                after = ()
        loss_sum = jnp.sum(jnp.concatenate(losses, axis=0), axis=1) / (inputs.shape[3] * dim)
        return results[0], results[1], loss_sum[None, None]

    grid_spec = P("tx", "ty")
    return jax.shard_map(device_train, mesh=mesh, in_specs=(grid_spec,) * 4, out_specs=(grid_spec,) * 3, check_vma=False)
```
